128 devices in a mesh: table: 32 (over x, y, core), batch: 4 (over z).
Axes of the slice: x: 4, y: 4, z: 4, core: 2. Of those that a mesh axis runs over, the one named last changes fastest.
Arguments:
- queries: bfloat16 [512, 4, 512], P(('table', 'batch')), may hold values from -5 to 5
- indices: int32 [512, 4, 32], P(('table', 'batch')), may hold values from 0 to 1048575, as said below
- first_keys: bfloat16 [4, 1024, 256], P(None, ('table', 'batch')), may hold values from -4 to 4
- second_keys: bfloat16 [4, 1024, 256], replicated, may hold values from -4 to 4
- values: bfloat16 [1048576, 1024], P(('table', 'batch')), may hold values from -6 to 6
Outputs:
- memory_read: bfloat16 [512, 1024], P(('table', 'batch'))
The draws below stay inside these ranges and needn't reach their ends.
Inputs may be any that keep to these rules, and one draw needn't show every extreme that they name: `indices`: row r of the value table belongs to device r // 8192 of table+batch. The entries of the 4 sequences of one device name rows of any one owner at most 8 times, and one owner is named exactly 8 times by the entries of every device.
All inputs are finite; a program needn't handle non-finite values.
Results may differ from the reference program's by a relative error of at most 0.005.
Values may be sent and summed in bfloat16 or wider, within the bound.
No kernel may reach another device: no remote copies, remote signals or barrier semaphores. Data moves between devices by JAX's collectives and lax.ppermute only.
A program may use at most 64 MiB of HBM per device.

```python
import math
import jax
import jax.numpy as jnp

HEADS = 4
KDIM = 512
HALF = 256
NSUB = 1024
DV = 1024
VALS_DEV = 8192
TOPK = 32
ROWS = 1048576
NFIRST = 1024
SEQS = 512
ENTRIES = 512
CAP = 8
DEVICES = 128


def owner_table(key):
    base_key = jax.random.fold_in(key, 101)
    hot_owner = jax.random.randint(jax.random.fold_in(base_key, 1), (), 0, DEVICES).astype(jnp.int32)
    others = (hot_owner + 1 + jnp.arange(DEVICES - 1, dtype=jnp.int32)) % DEVICES
    deck_cards = jnp.repeat(others, CAP)
    block_keys = jax.random.split(jax.random.fold_in(base_key, 2), DEVICES)

    def one_block(block_key):
        deal_key, mix_key, row_key = jax.random.split(block_key, 3)
        dealt = jax.random.permutation(deal_key, deck_cards)[:ENTRIES - CAP]
        owners = jnp.concatenate([jnp.zeros((CAP,), jnp.int32) + hot_owner, dealt.astype(jnp.int32)])
        owners = jax.random.permutation(mix_key, owners)
        picked = jax.random.randint(row_key, (ENTRIES,), 0, VALS_DEV).astype(jnp.int32)
        return owners * VALS_DEV + picked
    blocks = jax.vmap(one_block)(block_keys)
    return blocks.reshape(SEQS, HEADS, TOPK).astype(jnp.int32)


def key_table(key, marker, count):
    sub_key = jax.random.fold_in(key, marker)
    drawn = jnp.clip(jax.random.normal(sub_key, (HEADS, count, HALF), jnp.float32), -4.0, 4.0)
    return drawn.astype(jnp.bfloat16)


def draw_indices(key, part):
    return owner_table(key)


def draw_first_keys(key, part):
    return key_table(key, 202, NFIRST)


def draw_second_keys(key, part):
    return key_table(key, 303, NSUB)


def draw_queries(key, part):
    drawn_key = jax.random.fold_in(key, 404)
    spread = 1.4 / math.sqrt(KDIM)
    entries = jnp.clip(jax.random.normal(drawn_key, (SEQS, HEADS, KDIM), jnp.float32), -6.0, 6.0) * spread
    return entries.astype(jnp.bfloat16)


def level_of(stream_key, extent, shards, low, top_value):
    level = 1.0
    for position, blocks in shards:
        draws = jax.random.uniform(jax.random.fold_in(jax.random.fold_in(stream_key, 6), position), (blocks,), jnp.float32, low / len(shards), top_value / len(shards))
        level = level * jnp.repeat(jnp.exp(draws), extent[position] // blocks).reshape((-1,) + (1,) * (len(extent) - 1 - position))
    return level


def noise(own_key, extent, deviation, bound, cuts=(), held_as=jnp.bfloat16):
    values = deviation * jax.random.normal(own_key, extent, jnp.float32)
    if cuts:
        values = values * level_of(own_key, extent, cuts, -0.22, 0.18)
    return jnp.clip(values, -bound, bound).astype(held_as)


def setup_inputs(seed: int = 0) -> dict:
    key_list = jax.random.split(jax.random.key(seed), 6)
    return {
        "queries": draw_queries(jax.random.fold_in(key_list[5], 71), 0),
        "indices": draw_indices(jax.random.fold_in(key_list[5], 71), 0),
        "first_keys": draw_first_keys(jax.random.fold_in(key_list[5], 71), 0),
        "second_keys": draw_second_keys(jax.random.fold_in(key_list[5], 71), 0),
        "values": noise(key_list[4], (ROWS, DV), 1.0, 6.0, ((0, 128),)),
    }


def reference(queries, indices, first_keys, second_keys, values):
    head_ids = jnp.arange(HEADS, dtype=jnp.int32)[None, :, None]
    first_ids = (indices // NSUB).astype(jnp.int32)
    second_ids = (indices % NSUB).astype(jnp.int32)
    query_first = queries[:, :, :HALF].astype(jnp.float32)
    query_second = queries[:, :, HALF:].astype(jnp.float32)
    first_rows = first_keys[head_ids, first_ids].astype(jnp.float32)
    second_rows = second_keys[head_ids, second_ids].astype(jnp.float32)
    first_part = jnp.sum(query_first[:, :, None, :] * first_rows, axis=-1)
    second_part = jnp.sum(query_second[:, :, None, :] * second_rows, axis=-1)
    weights = jax.nn.softmax(first_part + second_part, axis=-1).astype(jnp.bfloat16)
    result = jnp.zeros((SEQS, DV), jnp.float32)
    for head_index in range(HEADS):
        fetched = values[indices[:, head_index]].astype(jnp.float32)
        result = result + jnp.einsum("sk,skd->sd", weights[:, head_index].astype(jnp.float32), fetched)
    return result.astype(jnp.bfloat16)
```

```python
import jax
import jax.numpy as jnp
from jax import lax
from jax.experimental import pallas as pl
from jax.experimental.pallas import tpu as pltpu
from jax.sharding import Mesh, PartitionSpec as P

DEVICE_AXES = ("x", "y", "core", "z")
CHIP_AXES = ("x", "y", "z")
OWNER_AXES = ("core", "x", "y", "z")

SEQS = 4
HEADS = 4
TOPK = 32
GROUPS = SEQS * HEADS
ENTRIES = GROUPS * TOPK
HALF = 256
SUBS = 1024
KEYS_DEV = 8
CHIPS = 64
DEVICES = 128
VALS_DEV = 8192
DV = 1024
CAP = 8
LANES = 128
MIB = 1024 * 1024
ROW_LANE = 64
TILE = 8
NT = (((1,), (1,)), ((), ()))
NN = (((1,), (0,)), ((), ()))


def dot(a, b, dims):
    return lax.dot_general(a, b, dims, preferred_element_type=jnp.float32)


def iota(shape, axis):
    return lax.broadcasted_iota(jnp.int32, shape, axis)


def exchange(slots, axes):
    return lax.all_to_all(slots, axes, split_axis=0, concat_axis=0, tiled=True)


def picked(line, where):
    width = line.shape[1]
    total = jnp.zeros((TOPK, LANES), jnp.float32)
    for tile in range(width // LANES):
        lanes = iota((TOPK, LANES), 1) + tile * LANES
        part = jnp.broadcast_to(line[:, tile * LANES : (tile + 1) * LANES], (TOPK, LANES))
        total = total + jnp.where(lanes == where, part, 0.0)
    return jnp.sum(total, axis=1, keepdims=True)


def plan_kernel(
    core_ref, column_ref, line_ref, query_ref, keys_ref, second_ref, place_ref, rows_ref, lane_ref, owner_ref, scores
):
    core = core_ref[0]
    owners = line_ref[...] >> 13
    chips = ((owners >> 3) << 2) + (owners & 3)
    spots = ((owners >> 2) & 1) * CHIPS + chips
    owner_ref[...] = jnp.where(iota((DEVICES, ENTRIES), 0) == spots, 1.0, 0.0).astype(jnp.bfloat16)
    for head in range(HEADS):
        scores[head] = dot(query_ref[...], keys_ref[pl.ds(head * SUBS, SUBS), :], NT)
    for group in range(GROUPS):
        here = pl.ds(group * TOPK, TOPK)
        index = jnp.broadcast_to(column_ref[here, :], (TOPK, LANES))
        owner = index >> 13
        rank = jnp.zeros((TOPK, LANES), jnp.int32)
        for tile in range(ENTRIES // LANES):
            if tile * LANES > group * TOPK + TOPK - 1:
                continue
            other = jnp.broadcast_to(owners[:, tile * LANES : (tile + 1) * LANES], (TOPK, LANES))
            earlier = iota((TOPK, LANES), 1) + tile * LANES < iota((TOPK, LANES), 0) + group * TOPK
            rank = rank + jnp.where((other == owner) & earlier, 1, 0)
        rank = jnp.broadcast_to(
            jnp.sum(rank.astype(jnp.float32), axis=1, keepdims=True).astype(jnp.int32), (TOPK, LANES)
        )
        row = index & (VALS_DEV - 1)
        mark = row + 1
        lane = iota((TOPK, LANES), 1)
        slot_lane = lane == ROW_LANE + rank
        rows_ref[0, here, :] = jnp.where(slot_lane, (mark >> 6) << 6, 0).astype(jnp.float32).astype(jnp.bfloat16)
        rows_ref[1, here, :] = jnp.where(slot_lane, mark & 63, 0).astype(jnp.float32).astype(jnp.bfloat16)
        lane_ref[here, :] = (group // HEADS) * CAP + rank
        first = index >> 10
        chip = ((owner >> 3) << 2) + (owner & 3)
        away = jnp.where(((owner >> 2) & 1) == core, 0, 1)
        place_ref[here, :] = away * (CHIPS * KEYS_DEV) + chip * KEYS_DEV + (first & 7)
        line = scores[group % HEADS, pl.ds(group, 1), :]
        second_ref[here, :] = jnp.broadcast_to(picked(line, index & (SUBS - 1)), (TOPK, LANES))


def match_kernel(mine_ref, theirs_ref, keys_ref, mine_out, theirs_out):
    span = CHIPS * KEYS_DEV
    totals = [jnp.zeros((GROUPS, span), jnp.float32) for _ in range(2)]
    for head in range(HEADS):
        block = keys_ref[:, pl.ds(head * KEYS_DEV, KEYS_DEV), :].reshape(span, HALF)
        for side, ref in enumerate((mine_ref, theirs_ref)):
            found = dot(ref[...], block, NT)
            totals[side] = jnp.where(iota((GROUPS, span), 0) % HEADS == head, found, totals[side])
    mine_out[...] = totals[0]
    theirs_out[...] = totals[1]


def weigh_kernel(own_ref, away_ref, second_ref, place_ref, rows_ref, lane_ref, owner_ref, out_ref, weighed):
    span = CHIPS * KEYS_DEV
    for group in range(GROUPS):
        here = pl.ds(group * TOPK, TOPK)
        place = place_ref[here, :]
        line = pl.ds(group, 1)
        score = second_ref[here, :] + picked(own_ref[line, :], place) + picked(away_ref[line, :], place - span)
        raised = jnp.exp(score - jnp.max(score, axis=0, keepdims=True))
        weight = raised / jnp.sum(raised, axis=0, keepdims=True)
        hit = iota((TOPK, LANES), 1) == lane_ref[here, :]
        weighed[here, :] = jnp.where(hit, weight, 0.0).astype(jnp.bfloat16) + rows_ref[0, here, :]
    owner = owner_ref[...]
    total = dot(owner, weighed[...], NN) + dot(owner, rows_ref[1], NN)
    out_ref[:, 0, :] = total


def fetch_kernel(side_ref, mail_ref, values_ref, out_ref, row_words, row_spots, tiles, mixes, spot_sem, sems):
    blocks = 4
    side = side_ref[0]
    mail = mail_ref[pl.ds(side * CHIPS, CHIPS), 0, :]
    marks = mail.astype(jnp.int32)
    spare = iota((CHIPS, LANES), 0) * (CAP * TILE) + (iota((CHIPS, LANES), 1) & (CAP - 1)) * TILE
    rows = jnp.where(marks > 0, marks - 1, spare)
    row_words[...] = rows
    spots = pltpu.make_async_copy(row_words, row_spots, spot_sem)
    spots.start()
    spots.wait()
    chips_block = CHIPS // blocks
    rows_block = chips_block * CAP * TILE
    for block in range(blocks):

        def issue(step, carry, block=block):
            chip = block * chips_block + step
            for slot in range(CAP):
                row = row_spots[chip, ROW_LANE + slot]
                base = pl.multiple_of((row >> 3) << 3, TILE)
                spot = pl.multiple_of((chip * CAP + slot) * TILE, TILE)
                pltpu.make_async_copy(
                    values_ref.at[pl.ds(base, TILE)], tiles.at[pl.ds(spot, TILE)], sems.at[block]
                ).start()
            return carry

        lax.fori_loop(0, chips_block, issue, 0)
    spread = jnp.where(iota((8 * CHIPS, CHIPS), 0) >> 3 == iota((8 * CHIPS, CHIPS), 1), 1.0, 0.0)
    wide = dot(spread.astype(jnp.bfloat16), mail.astype(jnp.bfloat16), NN)
    mine = iota((8 * CHIPS, LANES), 1) >> 3 == iota((8 * CHIPS, LANES), 0) & 3
    wide = jnp.where(mine, wide, 0.0).astype(jnp.bfloat16)
    slot_of = (iota((LANES, rows_block), 1) >> 3) & (CAP - 1)
    slot_from = iota((LANES, rows_block), 0)
    copies = jnp.where(slot_from & (CAP - 1) == slot_of, 1.0, 0.0).astype(jnp.bfloat16)
    mixes[...] = dot(wide, copies, NN).astype(jnp.bfloat16)
    row_lanes = iota((CHIPS, LANES), 1) >> 3 == ROW_LANE >> 3
    within = jnp.where(row_lanes, rows & (TILE - 1), 0).astype(jnp.float32).astype(jnp.bfloat16)
    within = dot(within, jnp.where(slot_from == slot_of + ROW_LANE, 1.0, 0.0).astype(jnp.bfloat16), NN)
    outs_block = 8 * chips_block
    lane_chip = iota((chips_block, rows_block), 1) >> 6
    same = iota((outs_block, rows_block), 0) >> 3 == iota((outs_block, rows_block), 1) >> 6
    upper = iota((outs_block, DV // 2), 0) & 4 == 0
    for block in range(blocks):
        here = within[block * chips_block : (block + 1) * chips_block]
        here = jnp.where(iota((chips_block, rows_block), 0) == lane_chip, here, 0.0)
        here = jnp.sum(here, axis=0, keepdims=True).astype(jnp.int32)
        match = jnp.broadcast_to(here, (outs_block, rows_block)) == iota((outs_block, rows_block), 1) & (TILE - 1)
        mix = mixes[pl.ds(block * outs_block, outs_block), :].astype(jnp.float32)
        mix = jnp.where(same & match, mix, 0.0).astype(jnp.bfloat16)
        there = pl.ds(block * rows_block, rows_block)
        pltpu.make_async_copy(values_ref.at[pl.ds(0, rows_block)], tiles.at[there], sems.at[block]).wait()
        total = dot(mix, tiles[there, :], NN)
        out_ref[pl.ds(block * outs_block, outs_block), :] = jnp.where(
            upper, total[:, : DV // 2], total[:, DV // 2 :]
        ).astype(jnp.bfloat16)


def finish_kernel(parts_ref, out_ref):
    total = jnp.zeros((8, DV // 2), jnp.float32)
    for chip in range(CHIPS):
        total = total + parts_ref[chip].astype(jnp.float32)
    out_ref[:, : DV // 2] = total[:4].astype(jnp.bfloat16)
    out_ref[:, DV // 2 :] = total[4:].astype(jnp.bfloat16)


VMEM = pl.BlockSpec(memory_space=pltpu.VMEM)
SMEM = pl.BlockSpec(memory_space=pltpu.SMEM)
ANYWHERE = pl.BlockSpec(memory_space=pl.ANY)


def shaped(shape, dtype):
    return jax.ShapeDtypeStruct(shape, dtype)


def partial_rows(side, mail, values):
    return pl.pallas_call(
        fetch_kernel,
        out_shape=shaped((8 * CHIPS, DV // 2), jnp.bfloat16),
        in_specs=[SMEM, VMEM, ANYWHERE],
        out_specs=VMEM,
        scratch_shapes=[
            pltpu.VMEM((CHIPS, LANES), jnp.int32),
            pltpu.SMEM((CHIPS, LANES), jnp.int32),
            pltpu.VMEM((CAP * CHIPS * TILE, DV), jnp.bfloat16),
            pltpu.VMEM((8 * CHIPS, CAP * CHIPS * TILE // 4), jnp.bfloat16),
            pltpu.SemaphoreType.DMA,
            pltpu.SemaphoreType.DMA((4,)),
        ],
        compiler_params=pltpu.CompilerParams(vmem_limit_bytes=50 * MIB),
        cost_estimate=pl.CostEstimate(flops=10**9, bytes_accessed=3 * 1024 * 1024, transcendentals=0),
    )(side, mail, values)


def swapped(x):
    return lax.ppermute(x, "core", [(0, 1), (1, 0)])


def memory_read(queries, indices, first_keys, second_keys, values):
    core = lax.axis_index("core").astype(jnp.int32).reshape(1)
    keys = jnp.broadcast_to(
        first_keys.reshape(1, HEADS * KEYS_DEV, HALF), (CHIPS, HEADS * KEYS_DEV, HALF)
    )
    keys = exchange(keys, CHIP_AXES)
    asked = queries.reshape(GROUPS, 2 * HALF)
    asked_first = asked[:, :HALF]
    theirs = swapped(asked_first)

    plan = pl.pallas_call(
        plan_kernel,
        out_shape=(
            shaped((ENTRIES, LANES), jnp.float32),
            shaped((ENTRIES, LANES), jnp.int32),
            shaped((2, ENTRIES, LANES), jnp.bfloat16),
            shaped((ENTRIES, LANES), jnp.int32),
            shaped((DEVICES, ENTRIES), jnp.bfloat16),
        ),
        in_specs=[SMEM, VMEM, VMEM, VMEM, VMEM],
        out_specs=(VMEM,) * 5,
        scratch_shapes=[pltpu.VMEM((HEADS, GROUPS, SUBS), jnp.float32)],
        cost_estimate=pl.CostEstimate(flops=2 * 10**9, bytes_accessed=3 * 1024 * 1024, transcendentals=0),
        compiler_params=pltpu.CompilerParams(vmem_limit_bytes=12 * MIB),
        name="plan",
    )(
        core,
        indices.reshape(ENTRIES, 1),
        indices.reshape(1, ENTRIES),
        asked[:, HALF:],
        second_keys.reshape(HEADS * SUBS, HALF),
    )
    second, place, rows, lane, owner = plan

    span = CHIPS * KEYS_DEV
    own, away = pl.pallas_call(
        match_kernel,
        out_shape=(shaped((GROUPS, span), jnp.float32),) * 2,
        in_specs=[VMEM] * 3,
        out_specs=(VMEM,) * 2,
        compiler_params=pltpu.CompilerParams(vmem_limit_bytes=10 * MIB),
        name="match",
    )(asked_first, theirs, keys)
    away = swapped(away)
    mail = pl.pallas_call(
        weigh_kernel,
        out_shape=shaped((DEVICES, 1, LANES), jnp.float32),
        in_specs=[VMEM] * 7,
        out_specs=VMEM,
        scratch_shapes=[pltpu.VMEM((ENTRIES, LANES), jnp.bfloat16)],
        compiler_params=pltpu.CompilerParams(vmem_limit_bytes=8 * MIB),
        name="weigh",
    )(own, away, second, place, rows, lane, owner)
    mail = exchange(mail, OWNER_AXES)

    passed = swapped(partial_rows(1 - core, mail, values))
    kept = partial_rows(core, mail, values)
    both = (kept.astype(jnp.float32) + passed.astype(jnp.float32)).astype(jnp.bfloat16)
    parts = exchange(both.reshape(CHIPS, 8, DV // 2), CHIP_AXES)
    return pl.pallas_call(
        finish_kernel,
        out_shape=shaped((SEQS, DV), jnp.bfloat16),
        in_specs=[VMEM],
        out_specs=VMEM,
        compiler_params=pltpu.CompilerParams(vmem_limit_bytes=8 * MIB),
        name="finish",
    )(parts)


def solution(mesh):
    chips = Mesh(mesh.devices.reshape(4, 4, 2, 4), DEVICE_AXES)
    return jax.shard_map(
        memory_read,
        mesh=chips,
        in_specs=(
            P(DEVICE_AXES, None, None),
            P(DEVICE_AXES, None, None),
            P(None, DEVICE_AXES, None),
            P(),
            P(DEVICE_AXES, None),
        ),
        out_specs=P(DEVICE_AXES, None),
        check_vma=False,
    )
```

```python
import jax
import jax.numpy as jnp
from jax import lax
from jax.experimental import pallas as pl
from jax.experimental.pallas import tpu as pltpu
from jax.sharding import Mesh, PartitionSpec as P

DEVICE_AXES = ("x", "y", "core", "half", "z")
CHIP_AXES = ("x", "y", "half", "z")
KEY_AXES = ("x", "y", "z")
OWNER_AXES = ("core", "x", "y", "half", "z")

SEQS = 4
HEADS = 4
TOPK = 32
GROUPS = SEQS * HEADS
ENTRIES = GROUPS * TOPK
HALF = 256
SUBS = 1024
KEYS_DEV = 8
CHIPS = 64
KEY_CHIPS = 32
QUARTER = KEY_CHIPS * KEYS_DEV
DEVICES = 128
VALS_DEV = 8192
DV = 1024
CAP = 8
LANES = 128
MIB = 1024 * 1024
ROW_LANE = 64
TILE = 8
AHEAD = 3
NT = (((1,), (1,)), ((), ()))
NN = (((1,), (0,)), ((), ()))


def dot(a, b, dims):
    return lax.dot_general(a, b, dims, preferred_element_type=jnp.float32)


def iota(shape, axis):
    return lax.broadcasted_iota(jnp.int32, shape, axis)


def exchange(slots, axes):
    return lax.all_to_all(slots, axes, split_axis=0, concat_axis=0, tiled=True)


def picked(line, where):
    width = line.shape[1]
    total = jnp.zeros((TOPK, LANES), jnp.float32)
    for tile in range(width // LANES):
        lanes = iota((TOPK, LANES), 1) + tile * LANES
        part = jnp.broadcast_to(line[:, tile * LANES : (tile + 1) * LANES], (TOPK, LANES))
        total = total + jnp.where(lanes == where, part, 0.0)
    return jnp.sum(total, axis=1, keepdims=True)


def repeat_kernel(keys_ref, out_ref):
    block = keys_ref[...]
    for chip in range(KEY_CHIPS):
        out_ref[chip] = block


def plan_kernel(
    here_ref,
    index_ref,
    query_ref,
    keys_ref,
    second_ref,
    place_ref,
    rows_ref,
    lane_ref,
    owner_ref,
    scores,
    keys,
    keys_sem,
):
    keys_copy = pltpu.make_async_copy(keys_ref, keys, keys_sem)
    keys_copy.start()
    flat = jnp.concatenate([index_ref[seq] for seq in range(SEQS)], axis=0)
    columns = flat.T
    owners = jnp.concatenate([flat[group : group + 1, :] for group in range(GROUPS)], axis=1) >> 13
    core = here_ref[0]
    half = here_ref[1]
    chips = ((owners >> 3) << 2) + (owners & 3)
    spots = ((owners >> 2) & 1) * CHIPS + chips
    owner_ref[...] = jnp.where(iota((DEVICES, ENTRIES), 0) == spots, 1.0, 0.0).astype(jnp.bfloat16)
    for group in range(GROUPS):
        here = pl.ds(group * TOPK, TOPK)
        index = jnp.broadcast_to(columns[:, group : group + 1], (TOPK, LANES))
        owner = index >> 13
        rank = jnp.zeros((TOPK, LANES), jnp.int32)
        for tile in range(ENTRIES // LANES):
            if tile * LANES > group * TOPK + TOPK - 1:
                continue
            other = jnp.broadcast_to(owners[:, tile * LANES : (tile + 1) * LANES], (TOPK, LANES))
            earlier = iota((TOPK, LANES), 1) + tile * LANES < iota((TOPK, LANES), 0) + group * TOPK
            rank = rank + jnp.where((other == owner) & earlier, 1, 0)
        rank = jnp.broadcast_to(
            jnp.sum(rank.astype(jnp.float32), axis=1, keepdims=True).astype(jnp.int32), (TOPK, LANES)
        )
        row = index & (VALS_DEV - 1)
        mark = row + 1
        lane = iota((TOPK, LANES), 1)
        slot_lane = lane == ROW_LANE + rank
        rows_ref[0, here, :] = jnp.where(slot_lane, (mark >> 6) << 6, 0).astype(jnp.float32).astype(jnp.bfloat16)
        rows_ref[1, here, :] = jnp.where(slot_lane, mark & 63, 0).astype(jnp.float32).astype(jnp.bfloat16)
        lane_ref[here, :] = (group // HEADS) * CAP + rank
        first = index >> 10
        chip = ((owner >> 3) << 1) + (owner & 1)
        away = jnp.where(((owner >> 2) & 1) == core, 0, 1) + jnp.where(((owner >> 1) & 1) == half, 0, 2)
        place_ref[here, :] = away * QUARTER + chip * KEYS_DEV + (first & 7)
    keys_copy.wait()
    for head in range(HEADS):
        scores[head] = dot(query_ref[...], keys[pl.ds(head * SUBS, SUBS), :], NT)
    for group in range(GROUPS):
        here = pl.ds(group * TOPK, TOPK)
        index = jnp.broadcast_to(columns[:, group : group + 1], (TOPK, LANES))
        line = scores[group % HEADS, pl.ds(group, 1), :]
        second_ref[here, :] = jnp.broadcast_to(picked(line, index & (SUBS - 1)), (TOPK, LANES))


def match_kernel(asked_0, asked_1, asked_2, asked_3, keys_ref, out_0, out_1, out_2, out_3):
    asked = jnp.concatenate([ref[...] for ref in (asked_0, asked_1, asked_2, asked_3)], axis=0)
    total = jnp.zeros((4 * GROUPS, QUARTER), jnp.float32)
    for head in range(HEADS):
        block = keys_ref[:, pl.ds(head * KEYS_DEV, KEYS_DEV), :].reshape(QUARTER, HALF)
        found = dot(asked, block, NT)
        total = jnp.where(iota((4 * GROUPS, QUARTER), 0) % HEADS == head, found, total)
    for side, ref in enumerate((out_0, out_1, out_2, out_3)):
        ref[...] = total[side * GROUPS : (side + 1) * GROUPS]


def weigh_kernel(
    part_0, part_1, part_2, part_3, second_ref, place_ref, rows_ref, lane_ref, owner_ref, out_ref, weighed
):
    for group in range(GROUPS):
        here = pl.ds(group * TOPK, TOPK)
        place = place_ref[here, :]
        line = pl.ds(group, 1)
        lines = [ref[line, :] for ref in (part_0, part_1, part_2, part_3)]
        score = second_ref[here, :] + picked(jnp.concatenate(lines, axis=1), place)
        raised = jnp.exp(score - jnp.max(score, axis=0, keepdims=True))
        weight = raised / jnp.sum(raised, axis=0, keepdims=True)
        hit = iota((TOPK, LANES), 1) == lane_ref[here, :]
        weighed[here, :] = jnp.where(hit, weight, 0.0).astype(jnp.bfloat16) + rows_ref[0, here, :]
    owner = owner_ref[...]
    total = dot(owner, weighed[...], NN) + dot(owner, rows_ref[1], NN)
    out_ref[:, 0, :] = total


def fetch_kernel(
    here_ref, mail_ref, values_ref, given_ref, kept_ref, row_words, row_spots, tiles, mixes, spot_sem, sems
):
    blocks = 8
    core = here_ref[0]
    mail = jnp.concatenate(
        [mail_ref[pl.ds((1 - core) * CHIPS, CHIPS), 0, :], mail_ref[pl.ds(core * CHIPS, CHIPS), 0, :]], axis=0
    )
    marks = mail.astype(jnp.int32)
    spare = iota((DEVICES, LANES), 0) * (CAP * TILE) + (iota((DEVICES, LANES), 1) & (CAP - 1)) * TILE
    rows = jnp.where(marks > 0, marks - 1, spare)
    row_words[...] = (rows - (rows & (TILE - 1))).T[ROW_LANE : ROW_LANE + CAP, :]
    spots = pltpu.make_async_copy(row_words, row_spots, spot_sem)
    spots.start()
    spots.wait()
    chips_block = DEVICES // blocks

    def issue(block):
        for chip in range(block * chips_block, (block + 1) * chips_block):
            for slot in range(CAP):
                base = pl.multiple_of(row_spots[slot, chip], TILE)
                spot = (chip * CAP + slot) * TILE
                pltpu.make_async_copy(
                    values_ref.at[pl.ds(base, TILE)], tiles.at[pl.ds(spot, TILE)], sems.at[block]
                ).start()

    for block in range(AHEAD):
        issue(block)
    octet = iota((DEVICES, LANES), 1) >> 3
    kept = jnp.where(octet == ROW_LANE >> 3, (rows & (TILE - 1)).astype(jnp.float32), mail)
    kept = jnp.where(octet > ROW_LANE >> 3, 0.0, kept).astype(jnp.bfloat16)
    tall = (8 * DEVICES, LANES)
    spread = jnp.where(iota(tall, 0) >> 3 == iota(tall, 1), 1.0, 0.0).astype(jnp.bfloat16)
    wide = dot(spread, kept, NN)
    octet = iota(tall, 1) >> 3
    weights = jnp.where(octet == iota(tall, 0) & 3, wide, 0.0).astype(jnp.bfloat16)
    within = jnp.where(octet == ROW_LANE >> 3, wide, 0.0).astype(jnp.bfloat16)
    square = (LANES, LANES)
    expand = jnp.where(iota(square, 0) & (CAP - 1) == (iota(square, 1) >> 3) & (CAP - 1), 1.0, 0.0)
    expand = expand.astype(jnp.bfloat16)
    weights = dot(weights, expand, NN)
    within = dot(within, expand, NN).astype(jnp.int32)
    wanted = (within == iota(tall, 1) & (TILE - 1)) & (iota(tall, 1) >> 6 == (iota(tall, 0) >> 3) & 1)
    mixes[...] = jnp.where(wanted, weights, 0.0).astype(jnp.bfloat16)
    upper = iota((32, DV // 2), 0) & 4 == 0
    lower = iota((32, LANES), 0) < 16
    rows_block = chips_block * CAP * TILE
    none = jnp.zeros((32, LANES), jnp.bfloat16)
    for block in range(blocks):
        there = pl.ds(block * rows_block, rows_block)
        pltpu.make_async_copy(values_ref.at[pl.ds(0, rows_block)], tiles.at[there], sems.at[block]).wait()
        if block + AHEAD < blocks:
            issue(block + AHEAD)
        for quad in range(block * chips_block // 4, (block + 1) * chips_block // 4):
            mix = mixes[pl.ds(quad * 32, 32), :]
            mix = jnp.concatenate([jnp.where(lower, mix, none), jnp.where(lower, none, mix)], axis=1)
            total = dot(mix, tiles[pl.ds(quad * 256, 256), :], NN)
            total = jnp.where(upper, total[:, : DV // 2], total[:, DV // 2 :])
            if quad < CHIPS // 4:
                given_ref[pl.ds(quad * 32, 32), :] = total.astype(given_ref.dtype)
            else:
                kept_ref[pl.ds((quad - CHIPS // 4) * 32, 32), :] = total


def finish_kernel(parts_ref, out_ref):
    total = jnp.zeros((8, DV // 2), jnp.float32)
    for chip in range(CHIPS):
        total = total + parts_ref[chip].astype(jnp.float32)
    out_ref[:, : DV // 2] = total[:4].astype(jnp.bfloat16)
    out_ref[:, DV // 2 :] = total[4:].astype(jnp.bfloat16)


VMEM = pl.BlockSpec(memory_space=pltpu.VMEM)
SMEM = pl.BlockSpec(memory_space=pltpu.SMEM)
ANYWHERE = pl.BlockSpec(memory_space=pl.ANY)


def shaped(shape, dtype):
    return jax.ShapeDtypeStruct(shape, dtype)


def partial_rows(here, mail, values):
    return pl.pallas_call(
        fetch_kernel,
        out_shape=(
            shaped((8 * CHIPS, DV // 2), jnp.bfloat16),
            shaped((8 * CHIPS, DV // 2), jnp.float32),
        ),
        in_specs=[SMEM, VMEM, ANYWHERE],
        out_specs=(VMEM, VMEM),
        scratch_shapes=[
            pltpu.VMEM((CAP, DEVICES), jnp.int32),
            pltpu.SMEM((CAP, DEVICES), jnp.int32),
            pltpu.VMEM((CAP * DEVICES * TILE, DV), jnp.bfloat16),
            pltpu.VMEM((8 * DEVICES, LANES), jnp.bfloat16),
            pltpu.SemaphoreType.DMA,
            pltpu.SemaphoreType.DMA((8,)),
        ],
        compiler_params=pltpu.CompilerParams(vmem_limit_bytes=50 * MIB),
        cost_estimate=pl.CostEstimate(flops=10**9, bytes_accessed=20 * MIB, transcendentals=0),
        name="fetch",
    )(here, mail, values)


def swapped(x):
    return lax.ppermute(x, "core", [(0, 1), (1, 0)])


def mirrored(x):
    return lax.ppermute(x, ("half", "z"), [(z, 3 - z) for z in range(4)])


def opposed(x):
    return lax.ppermute(x, ("core", "half", "z"), [(i, 7 - i) for i in range(8)])


def memory_read(queries, indices, first_keys, second_keys, values):
    here = jnp.stack([lax.axis_index("core"), lax.axis_index("half")]).astype(jnp.int32)
    keys = pl.pallas_call(
        repeat_kernel,
        out_shape=shaped((KEY_CHIPS, HEADS * KEYS_DEV, HALF), jnp.bfloat16),
        in_specs=[VMEM],
        out_specs=VMEM,
        compiler_params=pltpu.CompilerParams(vmem_limit_bytes=4 * MIB),
        name="repeat",
    )(first_keys.reshape(HEADS * KEYS_DEV, HALF))
    keys = exchange(keys, KEY_AXES)
    asked = queries.reshape(GROUPS, 2 * HALF)
    asked_first = asked[:, :HALF]
    asked_all = (asked_first, swapped(asked_first), mirrored(asked_first), opposed(asked_first))

    plan = pl.pallas_call(
        plan_kernel,
        out_shape=(
            shaped((ENTRIES, LANES), jnp.float32),
            shaped((ENTRIES, LANES), jnp.int32),
            shaped((2, ENTRIES, LANES), jnp.bfloat16),
            shaped((ENTRIES, LANES), jnp.int32),
            shaped((DEVICES, ENTRIES), jnp.bfloat16),
        ),
        in_specs=[SMEM, VMEM, VMEM, ANYWHERE],
        out_specs=(VMEM,) * 5,
        scratch_shapes=[
            pltpu.VMEM((HEADS, GROUPS, SUBS), jnp.float32),
            pltpu.VMEM((HEADS * SUBS, HALF), jnp.bfloat16),
            pltpu.SemaphoreType.DMA,
        ],
        cost_estimate=pl.CostEstimate(flops=2 * 10**9, bytes_accessed=3 * 1024 * 1024, transcendentals=0),
        compiler_params=pltpu.CompilerParams(vmem_limit_bytes=12 * MIB),
        name="plan",
    )(
        here,
        indices,
        asked[:, HALF:],
        pltpu.with_memory_space_constraint(second_keys.reshape(HEADS * SUBS, HALF), pltpu.HBM),
    )
    second, place, rows, lane, owner = plan

    found = pl.pallas_call(
        match_kernel,
        out_shape=(shaped((GROUPS, QUARTER), jnp.float32),) * 4,
        in_specs=[VMEM] * 5,
        out_specs=(VMEM,) * 4,
        compiler_params=pltpu.CompilerParams(vmem_limit_bytes=8 * MIB),
        name="match",
    )(*asked_all, keys)
    found = (found[0], swapped(found[1]), mirrored(found[2]), opposed(found[3]))
    mail = pl.pallas_call(
        weigh_kernel,
        out_shape=shaped((DEVICES, 1, LANES), jnp.float32),
        in_specs=[VMEM] * 9,
        out_specs=VMEM,
        scratch_shapes=[pltpu.VMEM((ENTRIES, LANES), jnp.bfloat16)],
        compiler_params=pltpu.CompilerParams(vmem_limit_bytes=8 * MIB),
        name="weigh",
    )(*found, second, place, rows, lane, owner)
    mail = exchange(mail, OWNER_AXES)

    given, kept = partial_rows(here, mail, values)
    both = (kept + swapped(given).astype(jnp.float32)).astype(jnp.bfloat16)
    parts = exchange(both.reshape(CHIPS, 8, DV // 2), CHIP_AXES)
    return pl.pallas_call(
        finish_kernel,
        out_shape=shaped((SEQS, DV), jnp.bfloat16),
        in_specs=[VMEM],
        out_specs=VMEM,
        compiler_params=pltpu.CompilerParams(vmem_limit_bytes=8 * MIB),
        name="finish",
    )(parts)


def solution(mesh):
    chips = Mesh(mesh.devices.reshape(4, 4, 2, 2, 2), DEVICE_AXES)
    return jax.shard_map(
        memory_read,
        mesh=chips,
        in_specs=(
            P(DEVICE_AXES, None, None),
            P(DEVICE_AXES, None, None),
            P(None, DEVICE_AXES, None),
            P(),
            P(DEVICE_AXES, None),
        ),
        out_specs=P(DEVICE_AXES, None),
        check_vma=False,
    )
```

```python
import jax
import jax.numpy as jnp
from jax import lax
from jax.experimental import pallas as pl
from jax.experimental.pallas import tpu as pltpu
from jax.sharding import Mesh, PartitionSpec as P

DEVICE_AXES = ("x", "y", "core", "half", "z")
CHIP_AXES = ("x", "y", "half", "z")
KEY_AXES = ("x", "y", "z")
OWNER_AXES = ("core", "x", "y", "half", "z")

SEQS = 4
HEADS = 4
TOPK = 32
GROUPS = SEQS * HEADS
ENTRIES = GROUPS * TOPK
HALF = 256
SUBS = 1024
KEYS_DEV = 8
CHIPS = 64
KEY_CHIPS = 32
QUARTER = KEY_CHIPS * KEYS_DEV
DEVICES = 128
VALS_DEV = 8192
DV = 1024
CAP = 8
LANES = 128
MIB = 1024 * 1024
ROW_LANE = 64
TILE = 8
AHEAD = 3
BLOCKS = 8
NT = (((1,), (1,)), ((), ()))
NN = (((1,), (0,)), ((), ()))


def dot(a, b, dims):
    return lax.dot_general(a, b, dims, preferred_element_type=jnp.float32)


def iota(shape, axis):
    return lax.broadcasted_iota(jnp.int32, shape, axis)


def exchange(slots, axes):
    return lax.all_to_all(slots, axes, split_axis=0, concat_axis=0, tiled=True)


def picked(line, where):
    width = line.shape[1]
    total = jnp.zeros((TOPK, LANES), jnp.float32)
    for tile in range(width // LANES):
        lanes = iota((TOPK, LANES), 1) + tile * LANES
        part = jnp.broadcast_to(line[:, tile * LANES : (tile + 1) * LANES], (TOPK, LANES))
        total = total + jnp.where(lanes == where, part, 0.0)
    return jnp.sum(total, axis=1, keepdims=True)


def repeat_kernel(
    keys_ref, query_ref, index_ref, out_ref, first_ref, second_ref, flat_ref, keys, query, index, sems
):
    copies = [
        pltpu.make_async_copy(source, target, sems.at[at])
        for at, (source, target) in enumerate(((keys_ref, keys), (query_ref, query), (index_ref, index)))
    ]
    for copy in copies:
        copy.start()
    for copy in copies:
        copy.wait()
    block = keys[...]
    for chip in range(KEY_CHIPS):
        out_ref[chip] = block
    asked = jnp.concatenate([query[seq].astype(jnp.float32) for seq in range(SEQS)], axis=0)
    first_ref[...] = asked[:, :HALF].astype(jnp.bfloat16)
    second_ref[...] = asked[:, HALF:].astype(jnp.bfloat16)
    flat_ref[...] = jnp.concatenate([index[seq] for seq in range(SEQS)], axis=0)


def plan_kernel(
    here_ref,
    index_ref,
    query_ref,
    keys_ref,
    second_ref,
    place_ref,
    rows_ref,
    lane_ref,
    owner_ref,
    scores,
    keys,
    keys_sem,
):
    key_copies = []
    for head in range(HEADS):
        span = pl.ds(head * SUBS, SUBS)
        key_copies.append(pltpu.make_async_copy(keys_ref.at[span], keys.at[span], keys_sem.at[head]))
        key_copies[head].start()
    flat = index_ref[...]
    columns = flat.T
    owners = jnp.concatenate([flat[group : group + 1, :] for group in range(GROUPS)], axis=1) >> 13
    core = here_ref[0]
    half = here_ref[1]
    chips = ((owners >> 3) << 2) + (owners & 3)
    spots = ((owners >> 2) & 1) * CHIPS + chips
    owner_ref[...] = jnp.where(iota((DEVICES, ENTRIES), 0) == spots, 1.0, 0.0).astype(jnp.bfloat16)
    for group in range(GROUPS):
        here = pl.ds(group * TOPK, TOPK)
        index = jnp.broadcast_to(columns[:, group : group + 1], (TOPK, LANES))
        owner = index >> 13
        rank = jnp.zeros((TOPK, LANES), jnp.int32)
        for tile in range(ENTRIES // LANES):
            if tile * LANES > group * TOPK + TOPK - 1:
                continue
            other = jnp.broadcast_to(owners[:, tile * LANES : (tile + 1) * LANES], (TOPK, LANES))
            earlier = iota((TOPK, LANES), 1) + tile * LANES < iota((TOPK, LANES), 0) + group * TOPK
            rank = rank + jnp.where((other == owner) & earlier, 1, 0)
        rank = jnp.broadcast_to(
            jnp.sum(rank.astype(jnp.float32), axis=1, keepdims=True).astype(jnp.int32), (TOPK, LANES)
        )
        row = index & (VALS_DEV - 1)
        mark = row + 1
        lane = iota((TOPK, LANES), 1)
        slot_lane = lane == ROW_LANE + rank
        rows_ref[0, here, :] = jnp.where(slot_lane, (mark >> 6) << 6, 0).astype(jnp.float32).astype(jnp.bfloat16)
        rows_ref[1, here, :] = jnp.where(slot_lane, mark & 63, 0).astype(jnp.float32).astype(jnp.bfloat16)
        lane_ref[here, :] = (group // HEADS) * CAP + rank
        first = index >> 10
        chip = ((owner >> 3) << 1) + (owner & 1)
        away = jnp.where(((owner >> 2) & 1) == core, 0, 1) + jnp.where(((owner >> 1) & 1) == half, 0, 2)
        place_ref[here, :] = away * QUARTER + chip * KEYS_DEV + (first & 7)
    for head in range(HEADS):
        key_copies[head].wait()
        scores[head] = dot(query_ref[...], keys[pl.ds(head * SUBS, SUBS), :], NT)
    for group in range(GROUPS):
        here = pl.ds(group * TOPK, TOPK)
        index = jnp.broadcast_to(columns[:, group : group + 1], (TOPK, LANES))
        line = scores[group % HEADS, pl.ds(group, 1), :]
        second_ref[here, :] = jnp.broadcast_to(picked(line, index & (SUBS - 1)), (TOPK, LANES))


def match_kernel(asked_0, asked_1, asked_2, asked_3, keys_ref, out_0, out_1, out_2, out_3):
    asked = jnp.concatenate([ref[...] for ref in (asked_0, asked_1, asked_2, asked_3)], axis=0)
    total = jnp.zeros((4 * GROUPS, QUARTER), jnp.float32)
    for head in range(HEADS):
        block = keys_ref[:, pl.ds(head * KEYS_DEV, KEYS_DEV), :].reshape(QUARTER, HALF)
        found = dot(asked, block, NT)
        total = jnp.where(iota((4 * GROUPS, QUARTER), 0) % HEADS == head, found, total)
    for side, ref in enumerate((out_0, out_1, out_2, out_3)):
        ref[...] = total[side * GROUPS : (side + 1) * GROUPS]


def weigh_kernel(
    part_0, part_1, part_2, part_3, second_ref, place_ref, rows_ref, lane_ref, owner_ref, out_ref, weighed
):
    for group in range(GROUPS):
        here = pl.ds(group * TOPK, TOPK)
        place = place_ref[here, :]
        line = pl.ds(group, 1)
        lines = [ref[line, :] for ref in (part_0, part_1, part_2, part_3)]
        score = second_ref[here, :] + picked(jnp.concatenate(lines, axis=1), place)
        raised = jnp.exp(score - jnp.max(score, axis=0, keepdims=True))
        weight = raised / jnp.sum(raised, axis=0, keepdims=True)
        hit = iota((TOPK, LANES), 1) == lane_ref[here, :]
        weighed[here, :] = jnp.where(hit, weight, 0.0).astype(jnp.bfloat16) + rows_ref[0, here, :]
    owner = owner_ref[...]
    total = dot(owner, weighed[...], NN) + dot(owner, rows_ref[1], NN)
    out_ref[:, 0, :] = total


def fetch_kernel(
    here_ref, mail_ref, values_ref, given_ref, kept_ref, row_words, row_spots, tiles, mixes, spot_sem, sems
):
    blocks = BLOCKS
    core = here_ref[0]
    mail = jnp.concatenate(
        [mail_ref[pl.ds((1 - core) * CHIPS, CHIPS), 0, :], mail_ref[pl.ds(core * CHIPS, CHIPS), 0, :]], axis=0
    )
    marks = mail.astype(jnp.int32)
    spare = iota((DEVICES, LANES), 0) * (CAP * TILE) + (iota((DEVICES, LANES), 1) & (CAP - 1)) * TILE
    rows = jnp.where(marks > 0, marks - 1, spare)
    row_words[...] = (rows - (rows & (TILE - 1))).T[ROW_LANE : ROW_LANE + CAP, :]
    spots = pltpu.make_async_copy(row_words, row_spots, spot_sem)
    spots.start()
    octet = iota((DEVICES, LANES), 1) >> 3
    kept = jnp.where(octet == ROW_LANE >> 3, (rows & (TILE - 1)).astype(jnp.float32), mail)
    kept = jnp.where(octet > ROW_LANE >> 3, 0.0, kept).astype(jnp.bfloat16)
    tall = (8 * DEVICES, LANES)
    spread = jnp.where(iota(tall, 0) >> 3 == iota(tall, 1), 1.0, 0.0).astype(jnp.bfloat16)
    wide = dot(spread, kept, NN)
    spots.wait()
    chips_block = DEVICES // blocks

    def issue(block):
        for chip in range(block * chips_block, (block + 1) * chips_block):
            for slot in range(CAP):
                base = pl.multiple_of(row_spots[slot, chip], TILE)
                spot = (chip * CAP + slot) * TILE
                pltpu.make_async_copy(
                    values_ref.at[pl.ds(base, TILE)], tiles.at[pl.ds(spot, TILE)], sems.at[block]
                ).start()

    for block in range(AHEAD):
        issue(block)
    octet = iota(tall, 1) >> 3
    weights = jnp.where(octet == iota(tall, 0) & 3, wide, 0.0).astype(jnp.bfloat16)
    within = jnp.where(octet == ROW_LANE >> 3, wide, 0.0).astype(jnp.bfloat16)
    square = (LANES, LANES)
    expand = jnp.where(iota(square, 0) & (CAP - 1) == (iota(square, 1) >> 3) & (CAP - 1), 1.0, 0.0)
    expand = expand.astype(jnp.bfloat16)
    weights = dot(weights, expand, NN)
    within = dot(within, expand, NN).astype(jnp.int32)
    wanted = (within == iota(tall, 1) & (TILE - 1)) & (iota(tall, 1) >> 6 == (iota(tall, 0) >> 3) & 1)
    mixes[...] = jnp.where(wanted, weights, 0.0).astype(jnp.bfloat16)
    upper = iota((32, DV // 2), 0) & 4 == 0
    lower = iota((32, LANES), 0) < 16
    rows_block = chips_block * CAP * TILE
    none = jnp.zeros((32, LANES), jnp.bfloat16)
    for block in range(blocks):
        there = pl.ds(block * rows_block, rows_block)
        pltpu.make_async_copy(values_ref.at[pl.ds(0, rows_block)], tiles.at[there], sems.at[block]).wait()
        if block + AHEAD < blocks:
            issue(block + AHEAD)
        for quad in range(block * chips_block // 4, (block + 1) * chips_block // 4):
            mix = mixes[pl.ds(quad * 32, 32), :]
            mix = jnp.concatenate([jnp.where(lower, mix, none), jnp.where(lower, none, mix)], axis=1)
            total = dot(mix, tiles[pl.ds(quad * 256, 256), :], NN)
            total = jnp.where(upper, total[:, : DV // 2], total[:, DV // 2 :])
            if quad < CHIPS // 4:
                given_ref[pl.ds(quad * 32, 32), :] = total.astype(given_ref.dtype)
            else:
                kept_ref[pl.ds((quad - CHIPS // 4) * 32, 32), :] = total


def finish_kernel(parts_ref, out_ref):
    total = jnp.zeros((8, DV // 2), jnp.float32)
    for chip in range(CHIPS):
        total = total + parts_ref[chip].astype(jnp.float32)
    out_ref[:, : DV // 2] = total[:4].astype(jnp.bfloat16)
    out_ref[:, DV // 2 :] = total[4:].astype(jnp.bfloat16)


VMEM = pl.BlockSpec(memory_space=pltpu.VMEM)
SMEM = pl.BlockSpec(memory_space=pltpu.SMEM)
ANYWHERE = pl.BlockSpec(memory_space=pl.ANY)


def shaped(shape, dtype):
    return jax.ShapeDtypeStruct(shape, dtype)


def partial_rows(here, mail, values):
    return pl.pallas_call(
        fetch_kernel,
        out_shape=(
            shaped((8 * CHIPS, DV // 2), jnp.bfloat16),
            shaped((8 * CHIPS, DV // 2), jnp.float32),
        ),
        in_specs=[SMEM, VMEM, ANYWHERE],
        out_specs=(VMEM, VMEM),
        scratch_shapes=[
            pltpu.VMEM((CAP, DEVICES), jnp.int32),
            pltpu.SMEM((CAP, DEVICES), jnp.int32),
            pltpu.VMEM((CAP * DEVICES * TILE, DV), jnp.bfloat16),
            pltpu.VMEM((8 * DEVICES, LANES), jnp.bfloat16),
            pltpu.SemaphoreType.DMA,
            pltpu.SemaphoreType.DMA((BLOCKS,)),
        ],
        compiler_params=pltpu.CompilerParams(vmem_limit_bytes=50 * MIB),
        cost_estimate=pl.CostEstimate(flops=10**9, bytes_accessed=20 * MIB, transcendentals=0),
        name="fetch",
    )(here, mail, values)


def swapped(x):
    return lax.ppermute(x, "core", [(0, 1), (1, 0)])


def mirrored(x):
    return lax.ppermute(x, ("half", "z"), [(z, 3 - z) for z in range(4)])


def opposed(x):
    return lax.ppermute(x, ("core", "half", "z"), [(i, 7 - i) for i in range(8)])


def memory_read(queries, indices, first_keys, second_keys, values):
    here = jnp.stack([lax.axis_index("core"), lax.axis_index("half")]).astype(jnp.int32)
    in_hbm = [
        pltpu.with_memory_space_constraint(x, pltpu.HBM)
        for x in (first_keys.reshape(HEADS * KEYS_DEV, HALF), queries, indices)
    ]
    keys, asked_first, asked_second, flat = pl.pallas_call(
        repeat_kernel,
        out_shape=(
            shaped((KEY_CHIPS, HEADS * KEYS_DEV, HALF), jnp.bfloat16),
            shaped((GROUPS, HALF), jnp.bfloat16),
            shaped((GROUPS, HALF), jnp.bfloat16),
            shaped((GROUPS, TOPK), jnp.int32),
        ),
        in_specs=[ANYWHERE] * 3,
        out_specs=(VMEM,) * 4,
        scratch_shapes=[
            pltpu.VMEM((HEADS * KEYS_DEV, HALF), jnp.bfloat16),
            pltpu.VMEM((SEQS, HEADS, 2 * HALF), jnp.bfloat16),
            pltpu.VMEM((SEQS, HEADS, TOPK), jnp.int32),
            pltpu.SemaphoreType.DMA((3,)),
        ],
        compiler_params=pltpu.CompilerParams(vmem_limit_bytes=4 * MIB),
        name="repeat",
    )(*in_hbm)
    keys = exchange(keys, KEY_AXES)
    asked_all = (asked_first, swapped(asked_first), mirrored(asked_first), opposed(asked_first))

    plan = pl.pallas_call(
        plan_kernel,
        out_shape=(
            shaped((ENTRIES, LANES), jnp.float32),
            shaped((ENTRIES, LANES), jnp.int32),
            shaped((2, ENTRIES, LANES), jnp.bfloat16),
            shaped((ENTRIES, LANES), jnp.int32),
            shaped((DEVICES, ENTRIES), jnp.bfloat16),
        ),
        in_specs=[SMEM, VMEM, VMEM, ANYWHERE],
        out_specs=(VMEM,) * 5,
        scratch_shapes=[
            pltpu.VMEM((HEADS, GROUPS, SUBS), jnp.float32),
            pltpu.VMEM((HEADS * SUBS, HALF), jnp.bfloat16),
            pltpu.SemaphoreType.DMA((HEADS,)),
        ],
        cost_estimate=pl.CostEstimate(flops=2 * 10**9, bytes_accessed=3 * 1024 * 1024, transcendentals=0),
        compiler_params=pltpu.CompilerParams(vmem_limit_bytes=12 * MIB),
        name="plan",
    )(here, flat, asked_second, pltpu.with_memory_space_constraint(second_keys.reshape(HEADS * SUBS, HALF), pltpu.HBM))
    second, place, rows, lane, owner = plan

    found = pl.pallas_call(
        match_kernel,
        out_shape=(shaped((GROUPS, QUARTER), jnp.float32),) * 4,
        in_specs=[VMEM] * 5,
        out_specs=(VMEM,) * 4,
        compiler_params=pltpu.CompilerParams(vmem_limit_bytes=8 * MIB),
        name="match",
    )(*asked_all, keys)
    from_mirror = mirrored(found[2])
    from_opposite = opposed(found[3])
    from_pair = swapped(found[1])
    found = (found[0], from_pair, from_mirror, from_opposite)
    mail = pl.pallas_call(
        weigh_kernel,
        out_shape=shaped((DEVICES, 1, LANES), jnp.float32),
        in_specs=[VMEM] * 9,
        out_specs=VMEM,
        scratch_shapes=[pltpu.VMEM((ENTRIES, LANES), jnp.bfloat16)],
        compiler_params=pltpu.CompilerParams(vmem_limit_bytes=8 * MIB),
        name="weigh",
    )(*found, second, place, rows, lane, owner)
    mail = exchange(mail, OWNER_AXES)

    given, kept = partial_rows(here, mail, values)
    both = (kept + swapped(given).astype(jnp.float32)).astype(jnp.bfloat16)
    parts = exchange(both.reshape(CHIPS, 8, DV // 2), CHIP_AXES)
    return pl.pallas_call(
        finish_kernel,
        out_shape=shaped((SEQS, DV), jnp.bfloat16),
        in_specs=[VMEM],
        out_specs=VMEM,
        compiler_params=pltpu.CompilerParams(vmem_limit_bytes=8 * MIB),
        name="finish",
    )(parts)


def solution(mesh):
    chips = Mesh(mesh.devices.reshape(4, 4, 2, 2, 2), DEVICE_AXES)
    return jax.shard_map(
        memory_read,
        mesh=chips,
        in_specs=(
            P(DEVICE_AXES, None, None),
            P(DEVICE_AXES, None, None),
            P(None, DEVICE_AXES, None),
            P(),
            P(DEVICE_AXES, None),
        ),
        out_specs=P(DEVICE_AXES, None),
        check_vma=False,
    )
```
